32 devices in a mesh: dp: 1 (over z), ep: 32 (over y, x, core).
Axes of the slice: x: 4, y: 4, z: 1, core: 2. Of those that a mesh axis runs over, the one named last changes fastest.
The devices are a block of a 4x4x8 slice.
Arguments:
- hidden: bfloat16 [32768, 1024], P(('dp', 'ep'))
- route_idx: int32 [32768, 8], P(('dp', 'ep'))
- gate_weights: float32 [32768, 8], P(('dp', 'ep'))
- w_gate: bfloat16 [32, 1024, 512], P('ep')
- w_up: bfloat16 [32, 1024, 512], P('ep')
- w_down: bfloat16 [32, 512, 1024], P('ep')
Outputs:
- output: bfloat16 [32768, 1024], P(('dp', 'ep'))
All inputs are finite; a program needn't handle non-finite values.
Results may differ from the reference program's by a relative error of at most 0.001.
Values are sent between devices in bfloat16 or wider.
A program may use at most 768 MiB of HBM per device.

```python
import jax
import jax.numpy as jnp
from jax import lax

D_MODEL = 1024
D_FF = 512
EXPERTS = 32
TOP_K = 8
GROUP_SIZE = 32
TOKENS_DEV = 1024
ROW_CAP = 1024
HOT_EXPERTS = 2

COLD_EXPERTS = EXPERTS - HOT_EXPERTS
REST_SLOTS = TOKENS_DEV * TOP_K - HOT_EXPERTS * ROW_CAP
COLD_SPREAD = min(REST_SLOTS // COLD_EXPERTS - 1, ROW_CAP - (REST_SLOTS + COLD_EXPERTS - 1) // COLD_EXPERTS)
COLD_PAIRS = COLD_EXPERTS // 2
TOKENS_PART = GROUP_SIZE * TOKENS_DEV


def draw_routes(route_key):
    key_hot, key_src = jax.random.split(route_key)
    expert_order = jax.random.permutation(key_hot, EXPERTS)
    cold_pos = jnp.arange(COLD_EXPERTS)
    cold_base = (cold_pos + 1) * REST_SLOTS // COLD_EXPERTS - cold_pos * REST_SLOTS // COLD_EXPERTS
    hot_counts = jnp.full((HOT_EXPERTS,), ROW_CAP, jnp.int32)
    slot_seq = jnp.arange(TOKENS_DEV * TOP_K)

    def one_source(src_key):
        key_shift, key_cold, key_tok, key_rot = jax.random.split(src_key, 4)
        pair_shift = jax.random.randint(key_shift, (COLD_PAIRS,), 0, COLD_SPREAD + 1)
        count_delta = jnp.concatenate([jnp.stack([pair_shift, -pair_shift], axis=1).reshape(-1), jnp.zeros((COLD_EXPERTS - 2 * COLD_PAIRS,), jnp.int32)])
        cold_counts = (cold_base + count_delta)[jax.random.permutation(key_cold, COLD_EXPERTS)]
        block_ends = jnp.cumsum(jnp.concatenate([hot_counts, cold_counts]))
        seq_experts = expert_order[jnp.searchsorted(block_ends, slot_seq, side='right')]
        choice_table = seq_experts.reshape(TOP_K, TOKENS_DEV).T[jax.random.permutation(key_tok, TOKENS_DEV)]
        slot_shift = jax.random.randint(key_rot, (TOKENS_DEV, 1), 0, TOP_K)
        slot_cols = (jnp.arange(TOP_K)[None, :] + slot_shift) % TOP_K
        return jnp.take_along_axis(choice_table, slot_cols, axis=1)

    all_routes = jax.vmap(one_source)(jax.random.split(key_src, GROUP_SIZE))
    return all_routes.reshape(TOKENS_PART, TOP_K).astype(jnp.int32)


def setup_inputs(seed: int = 0, part: int = 0) -> dict:
    base_key = jax.random.key(seed)
    part_key = jax.random.fold_in(base_key, part)
    key_x, key_gate, key_route = jax.random.split(part_key, 3)
    key_wg, key_wu, key_wd = jax.random.split(jax.random.key(seed + 1), 3)
    hidden = jax.random.normal(key_x, (TOKENS_PART, D_MODEL), jnp.float32).astype(jnp.bfloat16)
    gate_weights = jax.random.uniform(key_gate, (TOKENS_PART, TOP_K), jnp.float32, 0.3, 0.7) * (2.0 / TOP_K)
    route_idx = draw_routes(key_route)
    w_gate = (jax.random.normal(key_wg, (EXPERTS, D_MODEL, D_FF), jnp.float32) * D_MODEL ** -0.5).astype(jnp.bfloat16)
    w_up = (jax.random.normal(key_wu, (EXPERTS, D_MODEL, D_FF), jnp.float32) * D_MODEL ** -0.5).astype(jnp.bfloat16)
    w_down = (jax.random.normal(key_wd, (EXPERTS, D_FF, D_MODEL), jnp.float32) * (2.0 * D_FF ** -0.5)).astype(jnp.bfloat16)
    return {'hidden': hidden, 'route_idx': route_idx, 'gate_weights': gate_weights, 'w_gate': w_gate, 'w_up': w_up, 'w_down': w_down}


def reference(hidden, route_idx, gate_weights, w_gate, w_up, w_down):
    expert_cap = GROUP_SIZE * ROW_CAP
    pair_count = TOKENS_PART * TOP_K
    flat_ids = route_idx.reshape(-1)
    sort_order = jnp.argsort(flat_ids, stable=True)
    counts = jnp.bincount(flat_ids, length=EXPERTS)
    starts = jnp.cumsum(counts) - counts
    slot_range = jnp.arange(expert_cap)
    pair_pos = jnp.minimum(starts[:, None] + slot_range[None, :], pair_count - 1)
    pair_ids = sort_order[pair_pos]
    is_valid = slot_range[None, :] < counts[:, None]
    tok_rows = pair_ids // TOP_K
    row_gates = jnp.where(is_valid, gate_weights.reshape(-1)[pair_ids], 0.0)

    def expert_step(y_accum, scan_items):
        tok_idx, gate_col, gate_mat, up_mat, down_mat = scan_items
        expert_in = hidden[tok_idx]
        gate_proj = jnp.dot(expert_in, gate_mat, preferred_element_type=jnp.float32)
        up_proj = jnp.dot(expert_in, up_mat, preferred_element_type=jnp.float32)
        hidden_act = (jax.nn.silu(gate_proj) * up_proj).astype(jnp.bfloat16)
        expert_out = jnp.dot(hidden_act, down_mat, preferred_element_type=jnp.float32).astype(jnp.bfloat16)
        y_accum = y_accum.at[tok_idx].add(gate_col[:, None] * expert_out.astype(jnp.float32))
        return y_accum, None

    y_total = lax.scan(expert_step, jnp.zeros((TOKENS_PART, D_MODEL), jnp.float32), (tok_rows, row_gates, w_gate, w_up, w_down))[0]
    return y_total.astype(jnp.bfloat16)
```

```python
import heapq
import math

import jax
import jax.numpy as jnp
from jax import lax
from jax.experimental import pallas as pl
from jax.experimental.pallas import tpu as pltpu
from jax.sharding import PartitionSpec as P

MESH = pl.DeviceIdType.MESH
BF16, F32 = jnp.bfloat16, jnp.float32
BOTH = (0, 1)
SIDES = (-1, 1)
DIRS = (1, -1)
GROUP = 4
LANES = 128
BLOCK = 2 * LANES
HELD = 16
PIECES = 32
ROWS = (0, 1, -1, 2)
CHUNKS = ((0, 256), (256, 256), (512, 256), (768, 128), (896, 128))
DETOUR = ()
LEAD = 12
SEGMENTS = (('o', LEAD), ('opp', LEAD - 2), ('op', 34 - 2 * LEAD), ('p', 2))
ORDER = ('W0', 'W1', 'G0', 'D0', 'T0', 'D1', 'd0', 'T1', 'R0', 'R1', 'd1', 'd2', 'd3', 'd4', 'P0', 'P1', 'P2', 'P3', 'P4',
         'F0', 'S0', 'F1', 'S1', 'f0', 's0', 'f1', 's1', 'f2', 's2', 'f3', 's3', 'f4', 's4')
RANK = {name: i for i, name in enumerate(ORDER)}
RATE, LATENCY, CHIP_RATE, CHIP_LATENCY = 45.6e3, 2.3, 400e3, 1.8
STEP_US, UNIT_US, FINAL_US, START_US, AHEAD_US = 1.28, 1.65, 0.6, 5.0, 4.0
NEVER, TICK_US = 1e9, 0.01


def make_steps():
    steps, base = [], {'o': 0, 'p': 0}
    for pattern, count in SEGMENTS:
        for ch in pattern * count:
            steps.append((ch, base[ch]))
            base[ch] += 1
    return steps


STEPS = make_steps()


class Planner:
    def __init__(self, piece_bytes, down_bytes, token_bytes, gate_bytes, sum_bytes):
        self.t, self.free, self.arr, self.ready, self.done, self.out = START_US, {}, {}, {}, set(), []
        self.piece, self.sum = piece_bytes, sum_bytes
        self.down = [down_bytes * w for _, w in CHUNKS]
        for n in SIDES:
            self.push(('x', n), gate_bytes, ('G', 0, n))
            for q in BOTH:
                self.push(('x', n), token_bytes, ('T', q, n))
            for k in BOTH:
                for d in DIRS:
                    for h in BOTH:
                        self.push(('x', n), piece_bytes, ('D', k, d, -n, h))
            for i, size in enumerate(self.down):
                for h in BOTH:
                    self.push(('x', n), size, ('d', i, -n, h))
        for h, d in zip(BOTH, DIRS):
            for k in BOTH:
                for part in BOTH:
                    self.push(('y', d), piece_bytes, ('W', k, d, part))
            for i in DETOUR:
                self.push(('y', d), self.down[i], ('w', i, h))

    def push(self, link, size, key):
        name, i, *_ = key
        queue = self.ready.setdefault(link, [])
        heapq.heappush(queue, (RANK.get(name + str(i), 0), len(self.arr) + len(queue) + len(self.out), size, key))

    def fill(self):
        for link, queue in self.ready.items():
            chip = link == 'chip'
            while queue and (chip or self.free.get(link, START_US) - self.t < AHEAD_US):
                _, _, size, key = heapq.heappop(queue)
                self.free[link] = max(self.t, self.free.get(link, START_US)) + size / (CHIP_RATE if chip else RATE)
                self.arr[key] = self.free[link] + (CHIP_LATENCY if chip else LATENCY)
                self.out.append(('send', key))

    def event(self, key):
        self.t = max(self.t, self.arr[key])
        self.out.append(('wait', key))
        self.done.add(key)
        t, i, *rest = key
        if t == 'W':
            d, h = rest
            for n in SIDES:
                self.push(('x', n), self.piece, ('R', i, d, -n, h))
        elif t in ('D', 'R', 'S', 'F'):
            d, n, h = rest
            if t == 'D':
                self.push(('y', -d), self.piece, ('S', i, d, n, h))
            if t == 'R':
                self.push(('y', d), self.piece, ('F', i, d, n, h))
            if (t, i, d, n, not h) in self.done:
                self.push('chip', 2 * self.piece, ('B', t, i, d, n))
        elif t == 'w':
            h, = rest
            for n in SIDES:
                self.push(('x', n), self.down[i], ('r', i, -n, h))
        elif t in ('d', 'r', 's', 'f'):
            n, *dy, h = rest
            d = DIRS[h]
            if t == 'd':
                for to in (-d,) if i in DETOUR else DIRS:
                    self.push(('y', to), self.down[i], ('s', i, n, -to, h))
                dy = 0
            elif t == 'f':
                dy = 2
            else:
                dy = dy[0] if dy else -d
                if dy == -d:
                    self.push(('y', d), self.down[i], ('f', i, n, h))
            self.done.add((i, n, dy, h))
            if (i, n, dy, not h) in self.done:
                self.push('chip', 2 * self.down[i], ('b', i, n, dy))
        self.fill()

    def next_event(self):
        waiting = [(a, k) for k, a in self.arr.items() if k not in self.done and k[0] not in 'BbTGP']
        return min(waiting, key=lambda z: z[0], default=None)

    def poll(self):
        self.fill()
        while (p := self.next_event()) and p[0] <= self.t:
            self.event(p[1])
        self.fill()

    def advance(self, upto=NEVER):
        p = self.next_event()
        c = [self.free.get(link, START_US) - AHEAD_US + TICK_US for link, queue in self.ready.items() if queue]
        self.t = max(self.t, min([p[0] if p else NEVER, upto] + c))
        self.poll()

    def need(self, key):
        while key not in self.done:
            if key[0] in 'BbTGP' and key in self.arr:
                if self.arr[key] <= self.t:
                    self.event(key)
                else:
                    self.advance(self.arr[key])
            else:
                self.advance()

    def have(self, keys):
        return all(k in self.done or self.arr.get(k, NEVER) <= self.t for k in keys)

    def spend(self, us):
        self.t += us
        self.poll()

    def take(self):
        out, self.out = self.out, []
        return out

    def run(self):
        pieces = [(t, k, d, n) for t in 'DRSF' for k in BOTH for d in DIRS for n in SIDES]
        order, evs1, evs2 = [], [], []
        self.poll()
        for s, (ch, a) in enumerate(STEPS):
            if ch == 'o':
                while not (c := [p for p in pieces if self.have([('B',) + p])]):
                    later = [self.arr[('B',) + p] for p in pieces if ('B',) + p in self.arr]
                    self.advance(min(later, default=NEVER))
                p = min(c, key=lambda z: self.arr[('B',) + z])
                pieces.remove(p)
                order.append(p)
                self.need(('B',) + p)
            elif a == 0:
                for n in SIDES:
                    for key in [('G', 0, n)] + [('T', q, n) for q in BOTH]:
                        self.need(key)
            evs1.append(self.take())
            if s:
                self.spend(STEP_US)
        loads = [(i, g) for i in range(len(CHUNKS)) for g in range(GROUP)]
        finals = list(range(len(CHUNKS)))

        def load(limit, force=None):
            while loads and loads[0][0] <= limit:
                i, g = loads[0]
                keys = [('b', i, n, ROWS[g]) for n in SIDES]
                if loads[0] != force and not self.have(keys):
                    break
                for key in keys:
                    self.need(key)
                self.out.append(('load', loads.pop(0)))

        def final(limit, force):
            while finals and finals[0] <= limit and (finals[0] <= force or self.have([('P', finals[0], n) for n in SIDES])):
                for n in SIDES:
                    self.need(('P', finals[0], n))
                self.out.append(('final', finals.pop(0)))
                self.t += FINAL_US

        load(1)
        evs1.append(self.take())
        self.spend(STEP_US)
        for i, (_, w) in enumerate(CHUNKS):
            for mine in BOTH:
                for g in range(GROUP):
                    load(i + 1)
                    if not mine and (i, g) in loads:
                        load(i + 1, (i, g))
                    if mine and not g:
                        for n in SIDES:
                            self.push(('x', n), self.sum * w, ('P', i, n))
                        self.poll()
                    if not mine and not g and i > 1:
                        self.out += [('reuse', ('P', i - 2, n)) for n in SIDES]
                    final(i - 1, i - 2 if mine else -1)
                    evs2.append(self.take())
                    self.spend(UNIT_US)
        final(len(CHUNKS), len(CHUNKS))
        return evs1, evs2, self.take(), order


def kernel(side, hid, idx, gate, wg, wu, wd, out, GU, WST, WDB, WDT,
           X, H, own, wbuf, WD, PS, RSB, G, GT, GPT, iv, gv,
           s_in, s_own, s_send, s_link, s_chip, s_way, s_tok, s_gate, s_down, s_dway, s_dchip, s_sum, s_w, s_wd, s_out):
    me = lax.axis_index('ep')
    core, x, y = lax.rem(me, 2), lax.rem(me // 2, side), me // (2 * side)
    tokens, d_model = hid.shape
    half, quarter = tokens // 2, tokens // 4
    ff = wd.shape[1]
    kh, fh = d_model // 2, ff // 2
    item = 2
    planner = Planner(kh * BLOCK * item, fh * item, quarter * d_model * item, HELD * half * 4, half * 4)
    evs1, evs2, tail, order = planner.run()
    rank = {p: i for i, p in enumerate(order)}

    def dev(dx, dy, dc=0):
        row, col = lax.rem(y + dy + side, side), lax.rem(x + dx + side, side)
        return {'ep': (row * side + col) * 2 + lax.rem(core + dc, 2)}

    def part(size, i):
        return pl.ds(i * size, size)

    def column(k, d):
        return (0 if d == 1 else 2) + k

    def expert(n, dy, cc=0):
        return ROWS.index(dy) * GROUP + (1 + n) + cc

    def chunk(i):
        c0, w = CHUNKS[i]
        return c0 // BLOCK, pl.ds(c0 % BLOCK, w)

    def down(i, e):
        b, c = chunk(i)
        return WDB.at[b, e, :, c]

    def down_half(i, n, dy, h):
        b, c = chunk(i)
        return WDB.at[b, expert(n, dy), part(fh, h), c]

    def piece(t, k, d, n, h):
        return GU.at[rank[t, k, d, n], 0, part(kh, h)]

    def copy_of(key, sem=None):
        t, i, *rest = key
        if t == 'G':
            n, = rest
            z = (1 - n) // 2
            return GT.at[part(HELD, 1), part(half, z)], GPT.at[:, part(half, z)], s_gate.at[z], (n, 0)
        if t == 'T':
            n, = rest
            z = (1 - n) + i
            return hid.at[part(quarter, z)], X.at[1, part(quarter, z)], s_tok.at[z], (n, 0)
        if t == 'W':
            d, h = rest
            j = column(i, d)
            return own.at[j, part(kh, h)], WST.at[j, part(kh, h)], s_way.at[j, h], (0, d)
        if t in ('D', 'R', 'S', 'F'):
            d, n, h = rest
            j = column(i, d)
            src, to = {'D': (own.at[j, part(kh, h)], (-n, 0)), 'R': (WST.at[j, part(kh, h)], (-n, 0)),
                       'S': (piece('D', i, d, n, h) if t == 'S' else None, (0, -d)),
                       'F': (piece('R', i, d, n, h) if t == 'F' else None, (0, d))}[t]
            return src, piece(t, i, d, n, h), s_link.at[rank[t, i, d, n], h], to
        if t == 'B':
            a = rank[(i, *rest)]
            return GU.at[a, 0], GU.at[a, 1], s_chip.at[a], (0, 0, 1)
        if t == 'w':
            h, = rest
            b, c = chunk(i)
            c0, w = CHUNKS[i]
            return wd.at[0, part(fh, h), pl.ds(c0, w)], WDT.at[b, part(fh, h), c], s_dway.at[i, h], (0, DIRS[h])
        if t in ('d', 'r', 's', 'f'):
            n, *dy, h = rest
            d = DIRS[h]
            b, c = chunk(i)
            c0, w = CHUNKS[i]
            if t == 'd':
                dy, src, to = 0, wd.at[0, part(fh, h), pl.ds(c0, w)], (-n, 0)
            elif t == 'r':
                dy, src, to = -d, WDT.at[b, part(fh, h), c], (-n, 0)
            elif t == 's':
                dy, = dy
                src, to = down_half(i, n, 0, h), (0, -dy)
            else:
                dy, src, to = 2, down_half(i, n, -d, h), (0, d)
            return src, down_half(i, n, dy, h), s_down.at[i, expert(n, dy) // 2, h], to
        if t == 'b':
            n, dy = rest
            return down(i, expert(n, dy)), down(i, expert(n, dy, 1)), s_dchip.at[i, expert(n, dy) // 2], (0, 0, 1)
        n, = rest
        z = (1 + n) // 2
        b, c = chunk(i)
        _, w = CHUNKS[i]
        return PS.at[1, i % 2, part(half, z), pl.ds(0, w)], RSB.at[b, part(half, z), c], s_sum.at[i, z], (n, 0)

    sent, settled = {}, set()

    def remote(key):
        src, dst, sem, to = copy_of(key)
        return pltpu.make_async_remote_copy(src, dst, s_send.at[sent[key]], sem, device_id=dev(*to), device_id_type=MESH)

    def stage(j, p):
        return pltpu.make_async_copy((wg, wu)[p].at[0, :, part(LANES, j)], own.at[j, :, part(LANES, p)], s_own.at[j, p])

    def bring(i):
        src, dst = ((hid, X.at[0]), (idx, iv), (gate, gv))[i]
        return pltpu.make_async_copy(src, dst, s_in.at[i])

    def tall(rows):
        return jnp.concatenate([rows, jnp.zeros((LANES - HELD, tokens), F32)], axis=0).T

    def build_gates():
        bring(1).wait()
        bring(2).wait()
        shape = (2 * HELD, tokens)
        r, t = lax.broadcasted_iota(jnp.int32, shape, 0), lax.broadcasted_iota(jnp.int32, shape, 1)
        e = lax.rem(r, HELD)
        q = e // GROUP
        dy = jnp.where(q == 1, 1, jnp.where(q == 2, -1, jnp.where(q == 3, 2, 0)))
        shift = jnp.where(r < HELD, 0, jnp.where(t < half, 1, -1)) + 2 * lax.rem(e // 2, 2) - 1
        row, col = lax.rem(y + dy + side, side), lax.rem(x + shift + side, side)
        ids = (row * side + col) * 2 + lax.rem(core + e, 2)
        acc = jnp.zeros(shape, F32)
        for c in range(idx.shape[0]):
            acc = acc + jnp.where(iv[c:c + 1, :] == ids, gv[c:c + 1, :], 0)
        GT[...] = acc
        G[0] = tall(acc[:HELD])

    flags = set()

    def first_time(name):
        new = name not in flags
        flags.add(name)
        return new

    def load_down(par, g, b, c, w):
        return pltpu.make_async_copy(WDB.at[b, part(GROUP, g), :, c], WD.at[par, part(GROUP, g), :, pl.ds(0, w)], s_wd.at[par, g])

    def store(i):
        c = pl.ds(*CHUNKS[i])
        return pltpu.make_async_copy(X.at[0, :, c], out.at[:, c], s_out.at[i])

    def emit(events):
        for kind, key in events:
            if kind == 'send':
                t, k, d, *_ = key
                if t in ('D', 'W') and first_time(column(k, d)):
                    for p in BOTH:
                        stage(column(k, d), p).wait()
                if t == 'G' and first_time('gates'):
                    build_gates()
                sent[key] = len(sent)
                remote(key).start()
            elif kind == 'wait':
                _, dst, sem, _ = copy_of(key)
                pltpu.make_async_copy(dst, dst, sem).wait()
                if key[0] == 'G' and not first_time('partner'):
                    G[1] = tall(GPT[...])
            elif kind == 'load':
                i, g = key
                b, c = chunk(i)
                load_down(i % 2, g, b, c, CHUNKS[i][1]).start()
            elif kind == 'reuse':
                remote(key).wait_send()
                settled.add(key)
            else:
                c0, w = CHUNKS[key]
                b, c = chunk(key)
                for r in range(0, tokens, BLOCK):
                    rows = pl.ds(r, BLOCK)
                    X[0, rows, pl.ds(c0, w)] = (PS[0, key % 2, rows, pl.ds(0, w)] + RSB[b, rows, c]).astype(BF16)
                store(key).start()

    barrier = pltpu.get_barrier_semaphore()
    near = [(1, 0), (-1, 0), (0, 1), (0, -1), (0, 0, 1)]
    for to in near:
        pl.semaphore_signal(barrier, inc=1, device_id=dev(*to), device_id_type=MESH)
    for k in BOTH:
        for d in DIRS:
            for p in BOTH:
                stage(column(k, d), p).start()
    for i in (1, 2, 0):
        bring(i).start()
    pl.semaphore_wait(barrier, len(near))

    def ffn_in(b, a, slot):
        for cc in BOTH:
            for r in range(0, tokens, BLOCK):
                rows = pl.ds(r, BLOCK)
                ab = jnp.dot(X[b, rows, :], wbuf[slot, cc], preferred_element_type=F32)
                u = ab[:, :LANES]
                H[b, a, cc, rows, :] = (u * jax.nn.sigmoid(u) * ab[:, LANES:]).astype(BF16)

    def load_piece(a, slot):
        return pltpu.make_async_copy(GU.at[a], wbuf.at[slot], s_w.at[slot])

    emit(evs1[0])
    bring(0).wait()
    load_piece(0, 0).start()
    first, base = 0, {'o': 0, 'p': 0}
    for si, (pattern, count) in enumerate(SEGMENTS):
        per = {ch: pattern.count(ch) for ch in base}
        after = {ch: base[ch] + per[ch] * count for ch in base}
        follow = SEGMENTS[si + 1][0][0] if si + 1 < len(SEGMENTS) else None

        def body(it, _, first=first, base=base, pattern=pattern, count=count, per=per, after=after, follow=follow):
            for j, ch in enumerate(pattern):
                t = first + it * len(pattern) + j
                a = base[ch] + it * per[ch] + pattern[:j].count(ch)
                for v in range(count):
                    if ev := evs1[first + v * len(pattern) + j + 1]:
                        pl.when(it == v)(lambda ev=ev: emit(ev))
                slot, other = lax.rem(t, 2), lax.rem(t + 1, 2)
                if nxt := pattern[j + 1:j + 2]:
                    load_piece(base[nxt] + it * per[nxt] + pattern[:j + 1].count(nxt), other).start()
                else:
                    nxt = pattern[0]
                    pl.when(it < count - 1)(lambda: load_piece(base[nxt] + (it + 1) * per[nxt], other).start())
                    if follow:
                        pl.when(it == count - 1)(lambda: load_piece(after[follow], other).start())
                load_piece(a, slot).wait()
                ffn_in(0 if ch == 'o' else 1, a, slot)
            return 0

        lax.fori_loop(0, count, body, 0)
        first, base = first + len(pattern) * count, after

    def held(n, dy):
        near_d, far_d = {0: 'DD', 1: 'SR', -1: 'RS', 2: 'FF'}[dy]
        return [rank[near_d, k, 1, n] for k in BOTH] + [rank[far_d, k, -1, n] for k in BOTH]

    def ffn_out(b, par, g, w):
        for q in range(GROUP):
            n, cc = SIDES[q // 2], q % 2
            e = g * GROUP + q
            for r in range(0, tokens, BLOCK):
                rows = pl.ds(r, BLOCK)
                hh = jnp.concatenate([H[b, a, cc, rows, :] for a in held(n, ROWS[g])], axis=1)
                o = jnp.dot(hh, WD[par, e, :, :w], preferred_element_type=F32).astype(BF16).astype(F32)
                ge = G[b, rows, e:e + 1]
                v = jnp.where(ge > 0, ge * o, 0)
                PS[b, par, rows, :w] = v if e == 0 else PS[b, par, rows, :w] + v

    runs = []
    for i, (_, w) in enumerate(CHUNKS):
        if runs and runs[-1][2] == w:
            runs[-1][1] += 1
        else:
            runs.append([i, 1, w])
    for start, count, w in runs:

        def body_down(ib, _, start=start, count=count, w=w):
            b = 1 - lax.rem(ib, 2)
            par = lax.rem(start + ib // 2, 2)
            for g in range(GROUP):
                for v in range(2 * count):
                    if ev := evs2[(2 * start + v) * GROUP + g]:
                        pl.when(ib == v)(lambda ev=ev: emit(ev))
                pl.when(b == 1)(lambda: load_down(par, g, 0, pl.ds(0, w), w).wait())
                ffn_out(b, par, g, w)
            return 0

        lax.fori_loop(0, 2 * count, body_down, 0)
    emit(tail)
    for key in sent:
        if key not in settled:
            remote(key).wait_send()
    for i in range(len(CHUNKS)):
        store(i).wait()


def solution(mesh):
    side = math.isqrt(mesh.shape['ep'] // 2)

    def device_body(hidden, route_idx, gate_weights, w_gate, w_up, w_down):
        tokens, d_model = hidden.shape
        ff = w_gate.shape[2]
        top_k = route_idx.shape[1]
        blocks, nc = d_model // BLOCK, len(CHUNKS)
        shape = jax.ShapeDtypeStruct
        anywhere = pl.BlockSpec(memory_space=pl.ANY)
        dma = pltpu.SemaphoreType.DMA
        columns = ff // LANES
        pairs = HELD // 2
        return pl.pallas_call(
            lambda *refs: kernel(side, *refs),
            out_shape=[shape((tokens, d_model), BF16), shape((PIECES, 2, d_model, BLOCK), BF16),
                       shape((columns, d_model, BLOCK), BF16), shape((blocks, HELD, ff, BLOCK), BF16),
                       shape((blocks, ff, BLOCK), BF16)],
            in_specs=[anywhere] * 6,
            out_specs=[anywhere] * 5,
            scratch_shapes=[
                pltpu.VMEM((2, tokens, d_model), BF16),
                pltpu.VMEM((2, PIECES, 2, tokens, LANES), BF16),
                pltpu.VMEM((columns, d_model, BLOCK), BF16),
                pltpu.VMEM((2, 2, d_model, BLOCK), BF16),
                pltpu.VMEM((2, HELD, ff, BLOCK), BF16),
                pltpu.VMEM((2, 2, tokens, BLOCK), F32),
                pltpu.VMEM((blocks, tokens, BLOCK), F32),
                pltpu.VMEM((2, tokens, LANES), F32),
                pltpu.VMEM((2 * HELD, tokens), F32),
                pltpu.VMEM((HELD, tokens), F32),
                pltpu.VMEM((top_k, tokens), jnp.int32),
                pltpu.VMEM((top_k, tokens), F32),
                dma((3,)), dma((columns, 2)), dma((256,)), dma((PIECES, 2)), dma((PIECES,)), dma((columns, 2)), dma((4,)),
                dma((2,)), dma((nc, pairs, 2)), dma((nc, 2)), dma((nc, pairs)), dma((nc, 2)), dma((2,)), dma((2, GROUP)),
                dma((nc,)),
            ],
            compiler_params=pltpu.CompilerParams(collective_id=0, has_side_effects=True, vmem_limit_bytes=67043328),
            name='moe',
        )(hidden, route_idx.T, gate_weights.T, w_gate, w_up, w_down)[0]

    row_spec = P(('dp', 'ep'), None)
    expert_spec = P('ep', None, None)
    return jax.shard_map(device_body, mesh=mesh, in_specs=(row_spec,) * 3 + (expert_spec,) * 3, out_specs=row_spec, check_vma=False)
```

```python
import heapq
import math

import jax
import jax.numpy as jnp
from jax import lax
from jax.experimental import pallas as pl
from jax.experimental.pallas import tpu as pltpu
from jax.sharding import PartitionSpec as P

MESH = pl.DeviceIdType.MESH
BF16, F32 = jnp.bfloat16, jnp.float32
BOTH = (0, 1)
SIDES = (-1, 1)
DIRS = (1, -1)
GROUP = 4
LANES = 128
BLOCK = 2 * LANES
HELD = 16
PIECES = 32
ROWS = (0, 1, -1, 2)
CHUNKS = ((0, 256), (256, 256), (512, 256), (768, 256))
DETOUR = (1,)
LEAD = 10
SEGMENTS = (('oo', LEAD // 2), ('opp', LEAD - 2), ('op', PIECES + 2 - 2 * LEAD), ('pp', 1))
SEGMENTS = tuple(z for z in SEGMENTS if z[1] > 0)
PARTS = ((0, 3), (3, 4))
ORDER = ('d0', 'G0', 'T1', 'D1', 'D0', 'T0', 'R0', 'R1', 'd1', 'd2', 'P0', 'P1', 'P2', 'P3', 'r1', 'd3', 's2', 's1',
         'W1', 'f3', 's0', 'f1', 'w1', 'S1', 'F1', 'f2', 'W0', 'S0', 'F0', 'f0', 's3')
RANK = {name: i for i, name in enumerate(ORDER)}
RATE, LATENCY, CHIP_RATE, CHIP_LATENCY, EVENT_US = 46.3e3, 2.8, 400e3, 1.8, 0.015
PAIR_US, EXPERT_US, DRAIN_US, FINAL_US, START_US, AHEAD_US = 1.09, 0.3, 0.2, 0.6, 5.0, 6.0
VMEM_BYTES = 64900000
NEVER, TICK_US = 1e9, 0.01


STEPS = [pattern for pattern, count in SEGMENTS for _ in range(count)]


class Planner:
    def __init__(self, piece_bytes, down_bytes, token_bytes, gate_bytes, sum_bytes):
        self.t, self.free, self.arr, self.ready, self.done, self.out = START_US, {}, {}, {}, set(), []
        self.piece, self.sum = piece_bytes, sum_bytes
        self.down = [down_bytes * w for _, w in CHUNKS]
        for n in SIDES:
            self.push(('x', n), gate_bytes, ('G', 0, n))
            for q in BOTH:
                self.push(('x', n), token_bytes, ('T', q, n))
            for k in BOTH:
                for d in DIRS:
                    for h in BOTH:
                        self.push(('x', n), piece_bytes, ('D', k, d, -n, h))
            for i, size in enumerate(self.down):
                for h in BOTH:
                    self.push(('x', n), size, ('d', i, -n, h))
        for h, d in zip(BOTH, DIRS):
            for k in BOTH:
                for part in BOTH:
                    self.push(('y', d), piece_bytes, ('W', k, d, part))
            for i in DETOUR:
                self.push(('y', d), self.down[i], ('w', i, h))

    def push(self, link, size, key):
        name, i, *_ = key
        queue = self.ready.setdefault(link, [])
        heapq.heappush(queue, (RANK.get(name + str(i), 0), len(self.arr) + len(queue) + len(self.out), size, key))

    def fill(self):
        for link, queue in self.ready.items():
            chip = link == 'chip'
            while queue and (chip or self.free.get(link, START_US) - self.t < AHEAD_US):
                _, _, size, key = heapq.heappop(queue)
                self.free[link] = max(self.t, self.free.get(link, START_US)) + size / (CHIP_RATE if chip else RATE)
                self.arr[key] = self.free[link] + (CHIP_LATENCY if chip else LATENCY)
                self.out.append(('send', key))
                self.t += EVENT_US

    def event(self, key):
        self.t = max(self.t, self.arr[key]) + EVENT_US
        self.out.append(('wait', key))
        self.done.add(key)
        t, i, *rest = key
        if t == 'W':
            d, h = rest
            for n in SIDES:
                self.push(('x', n), self.piece, ('R', i, d, -n, h))
        elif t in ('D', 'R', 'S', 'F'):
            d, n, h = rest
            if t == 'D':
                self.push(('y', -d), self.piece, ('S', i, d, n, h))
            if t == 'R':
                self.push(('y', d), self.piece, ('F', i, d, n, h))
            if (t, i, d, n, not h) in self.done:
                self.push('chip', 2 * self.piece, ('B', t, i, d, n))
        elif t == 'w':
            h, = rest
            for n in SIDES:
                self.push(('x', n), self.down[i], ('r', i, -n, h))
        elif t in ('d', 'r', 's', 'f'):
            n, *dy, h = rest
            d = DIRS[h]
            if t == 'd':
                for to in (-d,) if i in DETOUR else DIRS:
                    self.push(('y', to), self.down[i], ('s', i, n, -to, h))
                dy = 0
            elif t == 'f':
                dy = 2
            else:
                dy = dy[0] if dy else -d
                if dy == -d:
                    self.push(('y', d), self.down[i], ('f', i, n, h))
            self.done.add((i, n, dy, h))
            if (i, n, dy, not h) in self.done:
                self.push('chip', 2 * self.down[i], ('b', i, n, dy))
        self.fill()

    def next_event(self):
        waiting = [(a, k) for k, a in self.arr.items() if k not in self.done and k[0] not in 'BbTGP']
        return min(waiting, key=lambda z: z[0], default=None)

    def poll(self):
        self.fill()
        while (p := self.next_event()) and p[0] <= self.t:
            self.event(p[1])
        self.fill()

    def advance(self, upto=NEVER):
        p = self.next_event()
        c = [self.free.get(link, START_US) - AHEAD_US + TICK_US for link, queue in self.ready.items() if queue]
        self.t = max(self.t, min([p[0] if p else NEVER, upto] + c))
        self.poll()

    def need(self, key):
        while key not in self.done:
            if key[0] in 'BbTGP' and key in self.arr:
                if self.arr[key] <= self.t:
                    self.event(key)
                else:
                    self.advance(self.arr[key])
            else:
                self.advance()

    def have(self, keys):
        return all(k in self.done or self.arr.get(k, NEVER) <= self.t for k in keys)

    def spend(self, us):
        self.t += us
        self.poll()

    def take(self):
        out, self.out = self.out, []
        return out

    def run(self):
        pieces = [(t, k, d, n) for t in 'DRSF' for k in BOTH for d in DIRS for n in SIDES]
        order, evs1, evs2 = [], [], []
        self.poll()
        partner = False
        for s, pattern in enumerate(STEPS):
            for ch in pattern:
                if ch == 'o':
                    while not (c := [p for p in pieces if self.have([('B',) + p])]):
                        later = [self.arr[('B',) + p] for p in pieces if ('B',) + p in self.arr]
                        self.advance(min(later, default=NEVER))
                    p = min(c, key=lambda z: self.arr[('B',) + z])
                    pieces.remove(p)
                    order.append(p)
                    self.need(('B',) + p)
                elif not partner:
                    partner = True
                    for n in SIDES:
                        for key in [('G', 0, n)] + [('T', q, n) for q in BOTH]:
                            self.need(key)
            evs1.append(self.take())
            if s:
                self.spend(DRAIN_US + PAIR_US * len(STEPS[s - 1]))
        loads = [(i, g) for i in range(len(CHUNKS)) for g in range(GROUP)]
        finals = list(range(len(CHUNKS)))

        def load(limit, force=None):
            while loads and loads[0][0] <= limit:
                i, g = loads[0]
                keys = [('b', i, n, ROWS[g]) for n in SIDES]
                if (force is None or loads[0] > force) and not self.have(keys):
                    break
                for key in keys:
                    self.need(key)
                self.out.append(('load', loads.pop(0)))

        def final(limit, force):
            while finals and finals[0] <= limit and (finals[0] <= force or self.have([('P', finals[0], n) for n in SIDES])):
                for n in SIDES:
                    self.need(('P', finals[0], n))
                self.out.append(('final', finals.pop(0)))
                self.t += FINAL_US

        load(1)
        evs1.append(self.take())
        self.spend(DRAIN_US + PAIR_US * len(STEPS[-1]))
        for i, (_, w) in enumerate(CHUNKS):
            for mine in BOTH:
                for begin, end in PARTS:
                    load(i + 1)
                    if not mine and (i, end - 1) in loads:
                        load(i + 1, (i, end - 1))
                    if mine and not begin:
                        for n in SIDES:
                            self.push(('x', n), self.sum * w, ('P', i, n))
                        self.poll()
                    if not mine and not begin and i > 1:
                        for n in SIDES:
                            while ('P', i - 2, n) not in self.arr:
                                self.advance()
                            self.out.append(('reuse', ('P', i - 2, n)))
                    final(i - 1, i - 2 if mine else -1)
                    evs2.append(self.take())
                    self.spend(DRAIN_US + EXPERT_US * GROUP * (end - begin))
        final(len(CHUNKS), len(CHUNKS))
        return evs1, evs2, self.take(), order


def kernel(side, hid, idx, gate, wg, wu, wd, out, GU, WST, WDB, WDT,
           X, H, own, wbuf, WD, PS, RSB, G, GT, GPT, iv, gv,
           s_in, s_own, s_send, s_link, s_chip, s_way, s_tok, s_gate, s_down, s_dway, s_dchip, s_sum, s_w, s_wd):
    me = lax.axis_index('ep')
    core, x, y = lax.rem(me, 2), lax.rem(me // 2, side), me // (2 * side)
    tokens, d_model = hid.shape
    half, quarter = tokens // 2, tokens // 4
    ff = wd.shape[1]
    kh, fh = d_model // 2, ff // 2
    item = 2
    planner = Planner(kh * BLOCK * item, fh * item, quarter * d_model * item, HELD * half * 4, half * 4)
    evs1, evs2, tail, order = planner.run()
    rank = {p: i for i, p in enumerate(order)}

    def device(dx, dy, dc=0):
        row, col = lax.rem(y + dy + side, side), lax.rem(x + dx + side, side)
        return (row * side + col) * 2 + lax.rem(core + dc, 2)

    near = {to: device(*to) for to in ((1, 0), (-1, 0), (0, 1), (0, -1), (0, 0, 1))}

    def dev(*to):
        return {'ep': near[to]}

    def part(size, i):
        return pl.ds(i * size, size)

    def column(k, d):
        return (0 if d == 1 else 2) + k

    def expert(n, dy, cc=0):
        return ROWS.index(dy) * GROUP + (1 + n) + cc

    def chunk(i):
        c0, w = CHUNKS[i]
        return c0 // BLOCK, pl.ds(c0 % BLOCK, w)

    def down(i, e):
        b, c = chunk(i)
        return WDB.at[b, e, :, c]

    def down_half(i, n, dy, h):
        b, c = chunk(i)
        return WDB.at[b, expert(n, dy), part(fh, h), c]

    def piece(t, k, d, n, h):
        return GU.at[rank[t, k, d, n], 0, part(kh, h)]

    def copy_of(key, sem=None):
        t, i, *rest = key
        if t == 'G':
            n, = rest
            z = (1 - n) // 2
            return GT.at[part(HELD, 1), part(half, z)], GPT.at[:, part(half, z)], s_gate.at[z], (n, 0)
        if t == 'T':
            n, = rest
            z = (1 - n) + i
            return hid.at[part(quarter, z)], X.at[part(quarter, z)], s_tok.at[z], (n, 0)
        if t == 'W':
            d, h = rest
            j = column(i, d)
            return own.at[j, part(kh, h)], WST.at[j, part(kh, h)], s_way.at[j, h], (0, d)
        if t in ('D', 'R', 'S', 'F'):
            d, n, h = rest
            j = column(i, d)
            src, to = {'D': (own.at[j, part(kh, h)], (-n, 0)), 'R': (WST.at[j, part(kh, h)], (-n, 0)),
                       'S': (piece('D', i, d, n, h) if t == 'S' else None, (0, -d)),
                       'F': (piece('R', i, d, n, h) if t == 'F' else None, (0, d))}[t]
            return src, piece(t, i, d, n, h), s_link.at[rank[t, i, d, n], h], to
        if t == 'B':
            a = rank[(i, *rest)]
            return GU.at[a, 0], GU.at[a, 1], s_chip.at[a], (0, 0, 1)
        if t == 'w':
            h, = rest
            b, c = chunk(i)
            c0, w = CHUNKS[i]
            return wd.at[0, part(fh, h), pl.ds(c0, w)], WDT.at[b, part(fh, h), c], s_dway.at[i, h], (0, DIRS[h])
        if t in ('d', 'r', 's', 'f'):
            n, *dy, h = rest
            d = DIRS[h]
            b, c = chunk(i)
            c0, w = CHUNKS[i]
            if t == 'd':
                dy, src, to = 0, wd.at[0, part(fh, h), pl.ds(c0, w)], (-n, 0)
            elif t == 'r':
                dy, src, to = -d, WDT.at[b, part(fh, h), c], (-n, 0)
            elif t == 's':
                dy, = dy
                src, to = down_half(i, n, 0, h), (0, -dy)
            else:
                dy, src, to = 2, down_half(i, n, -d, h), (0, d)
            return src, down_half(i, n, dy, h), s_down.at[i, expert(n, dy) // 2, h], to
        if t == 'b':
            n, dy = rest
            return down(i, expert(n, dy)), down(i, expert(n, dy, 1)), s_dchip.at[i, expert(n, dy) // 2], (0, 0, 1)
        n, = rest
        z = (1 + n) // 2
        b, c = chunk(i)
        _, w = CHUNKS[i]
        return PS.at[1, i % 2, part(half, z), pl.ds(0, w)], RSB.at[b, part(half, z), c], s_sum.at[i, z], (n, 0)

    sends = [key for events in evs1 + evs2 + [tail] for kind, key in events if kind == 'send']
    sent, settled = {key: i for i, key in enumerate(sends)}, set()

    def remote(key):
        src, dst, sem, to = copy_of(key)
        return pltpu.make_async_remote_copy(src, dst, s_send.at[sent[key]], sem, device_id=dev(*to), device_id_type=MESH)

    def stage(j, p):
        return pltpu.make_async_copy((wg, wu)[p].at[0, :, part(LANES, j)], own.at[j, :, part(LANES, p)], s_own.at[j, p])

    def bring(i):
        src, dst = ((hid, out), (idx, iv), (gate, gv))[i]
        return pltpu.make_async_copy(src, dst, s_in.at[i])

    def tall(rows):
        return jnp.concatenate([rows, jnp.zeros((LANES - HELD, tokens), F32)], axis=0).T

    def build_gates():
        bring(1).wait()
        bring(2).wait()
        shape = (2 * HELD, tokens)
        r, t = lax.broadcasted_iota(jnp.int32, shape, 0), lax.broadcasted_iota(jnp.int32, shape, 1)
        e = lax.rem(r, HELD)
        q = e // GROUP
        dy = jnp.where(q == 1, 1, jnp.where(q == 2, -1, jnp.where(q == 3, 2, 0)))
        shift = jnp.where(r < HELD, 0, jnp.where(t < half, 1, -1)) + 2 * lax.rem(e // 2, 2) - 1
        row, col = lax.rem(y + dy + side, side), lax.rem(x + shift + side, side)
        ids = (row * side + col) * 2 + lax.rem(core + e, 2)
        acc = jnp.zeros(shape, F32)
        for c in range(idx.shape[0]):
            acc = acc + jnp.where(iv[c:c + 1, :] == ids, gv[c:c + 1, :], 0)
        GT[...] = acc
        G[0] = tall(acc[:HELD])

    flags = set()

    def first_time(name):
        new = name not in flags
        flags.add(name)
        return new

    def load_down(par, g, b, c, w):
        return pltpu.make_async_copy(WDB.at[b, part(GROUP, g), :, c], WD.at[par, part(GROUP, g), :, pl.ds(0, w)], s_wd.at[par, g])

    def emit(events):
        for kind, key in events:
            if kind == 'send':
                t, k, d, *_ = key
                if t in ('D', 'W') and first_time(column(k, d)):
                    for p in BOTH:
                        stage(column(k, d), p).wait()
                if t == 'G' and first_time('gates'):
                    build_gates()
                remote(key).start()
            elif kind == 'wait':
                _, dst, sem, _ = copy_of(key)
                pltpu.make_async_copy(dst, dst, sem).wait()
                if key[0] == 'G' and not first_time('partner'):
                    G[1] = tall(GPT[...])
            elif kind == 'load':
                i, g = key
                b, c = chunk(i)
                load_down(i % 2, g, b, c, CHUNKS[i][1]).start()
            elif kind == 'reuse':
                remote(key).wait_send()
                settled.add(key)
            else:
                c0, w = CHUNKS[key]
                b, c = chunk(key)
                for r in range(0, tokens, BLOCK):
                    rows = pl.ds(r, BLOCK)
                    out[rows, pl.ds(c0, w)] = (PS[0, key % 2, rows, pl.ds(0, w)] + RSB[b, rows, c]).astype(BF16)

    barrier = pltpu.get_barrier_semaphore()
    for to in near:
        pl.semaphore_signal(barrier, inc=1, device_id=dev(*to), device_id_type=MESH)
    for k in BOTH:
        for d in DIRS:
            for p in BOTH:
                stage(column(k, d), p).start()
    for i in (1, 2, 0):
        bring(i).start()
    pl.semaphore_wait(barrier, len(near))

    def ffn_in(b, a, slot, j):
        rows_in = (out, X)[b]
        for cc in BOTH:
            for r in range(0, tokens, BLOCK):
                rows = pl.ds(r, BLOCK)
                ab = jnp.dot(rows_in[rows, :], wbuf[slot, j, cc], preferred_element_type=F32)
                u = ab[:, :LANES]
                H[b, a, cc, rows, :] = (u * jax.nn.sigmoid(u) * ab[:, LANES:]).astype(BF16)

    def load_piece(a, slot, j):
        return pltpu.make_async_copy(GU.at[a], wbuf.at[slot, j], s_w.at[slot, j])

    def indices(pattern, it, base):
        return [base[ch] + it * pattern.count(ch) + pattern[:j].count(ch) for j, ch in enumerate(pattern)]

    def load_pieces(pattern, it, base, slot):
        for j, a in enumerate(indices(pattern, it, base)):
            load_piece(a, slot, j).start()

    emit(evs1[0])
    bring(0).wait()
    first, base = 0, {'o': 0, 'p': 0}
    load_pieces(STEPS[0], 0, base, 0)
    for si, (pattern, count) in enumerate(SEGMENTS):
        after = {ch: base[ch] + pattern.count(ch) * count for ch in base}
        follow = SEGMENTS[si + 1][0] if si + 1 < len(SEGMENTS) else None

        def body(it, _, first=first, base=base, pattern=pattern, count=count, after=after, follow=follow):
            slot, other = lax.rem(first + it, 2), lax.rem(first + it + 1, 2)
            for v in range(count):
                if ev := evs1[first + v + 1]:
                    pl.when(it == v)(lambda ev=ev: emit(ev))
            pl.when(it < count - 1)(lambda: load_pieces(pattern, it + 1, base, other))
            if follow:
                pl.when(it == count - 1)(lambda: load_pieces(follow, 0, after, other))
            mine = indices(pattern, it, base)
            for j, a in enumerate(mine):
                load_piece(a, slot, j).wait()
            for j, (ch, a) in enumerate(zip(pattern, mine)):
                ffn_in(0 if ch == 'o' else 1, a, slot, j)
            return 0

        lax.fori_loop(0, count, body, 0)
        first, base = first + count, after

    def held(n, dy):
        near_d, far_d = {0: 'DD', 1: 'SR', -1: 'RS', 2: 'FF'}[dy]
        return [rank[near_d, k, 1, n] for k in BOTH] + [rank[far_d, k, -1, n] for k in BOTH]

    def ffn_out(b, par, g, w):
        for q in range(GROUP):
            n, cc = SIDES[q // 2], q % 2
            e = g * GROUP + q
            for r in range(0, tokens, BLOCK):
                rows = pl.ds(r, BLOCK)
                hh = jnp.concatenate([H[b, a, cc, rows, :] for a in held(n, ROWS[g])], axis=1)
                o = jnp.dot(hh, WD[par, e, :, :w], preferred_element_type=F32).astype(BF16).astype(F32)
                ge = G[b, rows, e:e + 1]
                v = jnp.where(ge > 0, ge * o, 0)
                PS[b, par, rows, :w] = v if e == 0 else PS[b, par, rows, :w] + v

    runs = []
    for i, (_, w) in enumerate(CHUNKS):
        if runs and runs[-1][2] == w:
            runs[-1][1] += 1
        else:
            runs.append([i, 1, w])
    for start, count, w in runs:

        def body_down(ib, _, start=start, count=count, w=w):
            b = 1 - lax.rem(ib, 2)
            par = lax.rem(start + ib // 2, 2)
            for z, (begin, end) in enumerate(PARTS):
                for v in range(2 * count):
                    if ev := evs2[(2 * start + v) * len(PARTS) + z]:
                        pl.when(ib == v)(lambda ev=ev: emit(ev))

                @pl.when(b == 1)
                def _():
                    for g in range(begin, end):
                        load_down(par, g, 0, pl.ds(0, w), w).wait()

                for g in range(begin, end):
                    ffn_out(b, par, g, w)
            return 0

        lax.fori_loop(0, 2 * count, body_down, 0)
    emit(tail)
    for key in sent:
        if key not in settled:
            remote(key).wait_send()


def solution(mesh):
    side = math.isqrt(mesh.shape['ep'] // 2)

    def device_body(hidden, route_idx, gate_weights, w_gate, w_up, w_down):
        tokens, d_model = hidden.shape
        ff = w_gate.shape[2]
        top_k = route_idx.shape[1]
        blocks, nc = d_model // BLOCK, len(CHUNKS)
        shape = jax.ShapeDtypeStruct
        anywhere = pl.BlockSpec(memory_space=pl.ANY)
        dma = pltpu.SemaphoreType.DMA
        columns = ff // LANES
        pairs = HELD // 2
        return pl.pallas_call(
            lambda *refs: kernel(side, *refs),
            out_shape=[pltpu.VMEM((tokens, d_model), BF16), shape((PIECES, 2, d_model, BLOCK), BF16),
                       shape((columns, d_model, BLOCK), BF16), shape((blocks, HELD, ff, BLOCK), BF16),
                       shape((blocks, ff, BLOCK), BF16)],
            in_specs=[anywhere] * 6,
            out_specs=[pl.BlockSpec(memory_space=pltpu.VMEM)] + [anywhere] * 4,
            scratch_shapes=[
                pltpu.VMEM((tokens, d_model), BF16),
                pltpu.VMEM((2, PIECES, 2, tokens, LANES), BF16),
                pltpu.VMEM((columns, d_model, BLOCK), BF16),
                pltpu.VMEM((2, 3, 2, d_model, BLOCK), BF16),
                pltpu.VMEM((2, HELD, ff, BLOCK), BF16),
                pltpu.VMEM((2, 2, tokens, BLOCK), F32),
                pltpu.VMEM((blocks, tokens, BLOCK), F32),
                pltpu.VMEM((2, tokens, LANES), F32),
                pltpu.VMEM((2 * HELD, tokens), F32),
                pltpu.VMEM((HELD, tokens), F32),
                pltpu.VMEM((top_k, tokens), jnp.int32),
                pltpu.VMEM((top_k, tokens), F32),
                dma((3,)), dma((columns, 2)), dma((256,)), dma((PIECES, 2)), dma((PIECES,)), dma((columns, 2)), dma((4,)),
                dma((2,)), dma((nc, pairs, 2)), dma((nc, 2)), dma((nc, pairs)), dma((nc, 2)), dma((2, 3)), dma((2, GROUP)),
            ],
            compiler_params=pltpu.CompilerParams(collective_id=0, has_side_effects=True, vmem_limit_bytes=VMEM_BYTES),
            name='moe',
        )(hidden, route_idx.T, gate_weights.T, w_gate, w_up, w_down)[0]

    row_spec = P(('dp', 'ep'), None)
    expert_spec = P('ep', None, None)
    return jax.shard_map(device_body, mesh=mesh, in_specs=(row_spec,) * 3 + (expert_spec,) * 3, out_specs=row_spec, check_vma=False)
```

```python
import heapq
import math

import jax
import jax.numpy as jnp
from jax import lax
from jax.experimental import pallas as pl
from jax.experimental.pallas import tpu as pltpu
from jax.sharding import PartitionSpec as P

MESH = pl.DeviceIdType.MESH
BF16, F32 = jnp.bfloat16, jnp.float32
BOTH = (0, 1)
SIDES = (-1, 1)
DIRS = (1, -1)
GROUP = 4
LANES = 128
BLOCK = 2 * LANES
HELD = 16
PIECES = 32
ROWS = (0, 1, -1, 2)
CHUNKS = ((0, 256), (256, 256), (512, 256), (768, 128), (896, 128))
TURNS = ((1, (0,)), (0, (0,)), (1, (1,)), (0, (1,)), (1, (2,)), (0, (2,)), (1, (3,)), (1, (4,)), (0, (3, 4)))
DETOUR = (0, 1, 2)
LEAD = 12
SEGMENTS = (('oo', LEAD // 2), ('opp', LEAD - 2), ('op', PIECES + 2 - 2 * LEAD), ('pp', 1))
SEGMENTS = tuple(z for z in SEGMENTS if z[1] > 0)
PARTS = ((0, 3), (3, 4))
ORDER = ('D0', 'G0', 'D1', 'T0', 'T1', 'R1', 'R0', 'd0', 'r0', 'd1', 'P0', 'P1', 'P2', 'P3', 'P4', 'r1', 'd2', 'r2',
         'd3', 'd4', 'W1', 'W0', 'F1', 'f3', 'w1', 's3', 'f0', 'f4', 'S1', 'w0', 'f1', 's4', 'S0', 's2', 'w2', 'F0',
         's1', 's0', 'f2')
RANK = {name: i for i, name in enumerate(ORDER)}
RATE, LATENCY, CHIP_RATE, CHIP_LATENCY, EVENT_US = 46.3e3, 2.8, 400e3, 1.8, 0.015
PAIR_US, EXPERT_US, DRAIN_US, FINAL_US, START_US, AHEAD_US = 1.13, 0.315, 0.22, 0.6, 5.0, 12.0
VMEM_BYTES = 64900000
NEVER, TICK_US, EARLY_US, SETTLED_US = 1e9, 0.01, 0.0, 3.0


def block(i):
    return CHUNKS[i][0] // BLOCK


STEPS = [pattern for pattern, count in SEGMENTS for _ in range(count)]


class Planner:
    def __init__(self, piece_bytes, down_bytes, token_bytes, gate_bytes, sum_bytes):
        self.t, self.free, self.arr, self.ready, self.done, self.out = START_US, {}, {}, {}, set(), []
        self.piece, self.sum, self.unsettled = piece_bytes, sum_bytes, []
        self.down = [down_bytes * w for _, w in CHUNKS]
        for n in SIDES:
            self.push(('x', n), gate_bytes, ('G', 0, n))
            for q in BOTH:
                self.push(('x', n), token_bytes, ('T', q, n))
            for k in BOTH:
                for d in DIRS:
                    for h in BOTH:
                        self.push(('x', n), piece_bytes, ('D', k, d, -n, h))
            for i, size in enumerate(self.down):
                for h in BOTH:
                    self.push(('x', n), size, ('d', i, -n, h))
        for h, d in zip(BOTH, DIRS):
            for k in BOTH:
                for part in BOTH:
                    self.push(('y', d), piece_bytes, ('W', k, d, part))
            for i in DETOUR:
                self.push(('y', d), self.down[i], ('w', i, h))

    def push(self, link, size, key):
        name, i, *_ = key
        queue = self.ready.setdefault(link, [])
        heapq.heappush(queue, (RANK.get(name + str(i), 0), len(self.arr) + len(queue) + len(self.out), size, key))

    def fill(self):
        for link, queue in self.ready.items():
            chip = link == 'chip'
            while queue and (chip or self.free.get(link, START_US) - self.t < AHEAD_US):
                _, _, size, key = heapq.heappop(queue)
                self.free[link] = max(self.t, self.free.get(link, START_US)) + size / (CHIP_RATE if chip else RATE)
                self.arr[key] = self.free[link] + (CHIP_LATENCY if chip else LATENCY)
                self.out.append(('send', key))
                self.t += EVENT_US
                if key[0] != 'P':
                    self.unsettled.append(key)

    def event(self, key):
        self.t = max(self.t, self.arr[key]) + EVENT_US
        self.out.append(('wait', key))
        self.done.add(key)
        t, i, *rest = key
        if t == 'W':
            d, h = rest
            for n in SIDES:
                self.push(('x', n), self.piece, ('R', i, d, -n, h))
        elif t in ('D', 'R', 'S', 'F'):
            d, n, h = rest
            if t == 'D':
                self.push(('y', -d), self.piece, ('S', i, d, n, h))
            if t == 'R':
                self.push(('y', d), self.piece, ('F', i, d, n, h))
            if (t, i, d, n, not h) in self.done:
                self.push('chip', 2 * self.piece, ('B', t, i, d, n))
        elif t == 'w':
            h, = rest
            for n in SIDES:
                self.push(('x', n), self.down[i], ('r', i, -n, h))
        elif t in ('d', 'r', 's', 'f'):
            n, *dy, h = rest
            d = DIRS[h]
            if t == 'd':
                for to in (-d,) if i in DETOUR else DIRS:
                    self.push(('y', to), self.down[i], ('s', i, n, -to, h))
                dy = 0
            elif t == 'f':
                dy = 2
            else:
                dy = dy[0] if dy else -d
                if dy == -d:
                    self.push(('y', d), self.down[i], ('f', i, n, h))
            self.done.add((i, n, dy, h))
            if (i, n, dy, not h) in self.done:
                self.push('chip', 2 * self.down[i], ('b', i, n, dy))
        self.fill()

    def next_event(self):
        waiting = [(a, k) for k, a in self.arr.items() if k not in self.done and k[0] not in 'BbTGP']
        return min(waiting, key=lambda z: z[0], default=None)

    def poll(self):
        self.fill()
        while (p := self.next_event()) and p[0] <= self.t:
            self.event(p[1])
        self.fill()

    def advance(self, upto=NEVER):
        while self.unsettled and self.arr[self.unsettled[0]] <= self.t - SETTLED_US:
            self.out.append(('settle', self.unsettled.pop(0)))
            self.t += EVENT_US
        p = self.next_event()
        c = [self.free.get(link, START_US) - AHEAD_US + TICK_US for link, queue in self.ready.items() if queue]
        self.t = max(self.t, min([p[0] if p else NEVER, upto] + c))
        self.poll()

    def need(self, key):
        while key not in self.done:
            if key[0] in 'BbTGP' and key in self.arr:
                if self.arr[key] <= self.t:
                    self.event(key)
                else:
                    self.advance(self.arr[key])
            else:
                self.advance()

    def have(self, keys, early=0.0):
        return all(k in self.done or self.arr.get(k, NEVER) <= self.t + early for k in keys)

    def spend(self, us):
        self.t += us
        self.poll()

    def take(self):
        out, self.out = self.out, []
        return out

    def run(self):
        pieces = [(t, k, d, n) for t in 'DRSF' for k in BOTH for d in DIRS for n in SIDES]
        order, evs1, evs2 = [], [], []
        self.poll()
        partner, reused = False, set()
        for s, pattern in enumerate(STEPS):
            for ch in pattern:
                if ch == 'o':
                    while not (c := [p for p in pieces if self.have([('B',) + p])]):
                        later = [self.arr[('B',) + p] for p in pieces if ('B',) + p in self.arr]
                        self.advance(min(later, default=NEVER))
                    p = min(c, key=lambda z: self.arr[('B',) + z])
                    pieces.remove(p)
                    order.append(p)
                    self.need(('B',) + p)
                elif not partner:
                    partner = True
                    for n in SIDES:
                        for key in [('G', 0, n)] + [('T', q, n) for q in BOTH]:
                            self.need(key)
            evs1.append(self.take())
            if s:
                self.spend(DRAIN_US + PAIR_US * len(STEPS[s - 1]))
        loads = [(i, g) for i in range(len(CHUNKS)) for g in range(GROUP)]
        finals, summed = list(range(len(CHUNKS))), set()

        def load(force=None):
            while loads:
                i, g = loads[0]
                keys = [('b', i, n, ROWS[g]) for n in SIDES]
                forced = force is not None and loads[0] <= force
                room = all(c in summed for c in range(i) if block(c) <= block(i) - 2)
                if not room or not (forced or self.have(keys, EARLY_US)):
                    break
                for key in keys:
                    self.need(key)
                self.out.append(('load', loads.pop(0)))

        def final(force=-1):
            while finals and finals[0] in summed and (finals[0] <= force or self.have([('P', finals[0], n) for n in SIDES])):
                for n in SIDES:
                    self.need(('P', finals[0], n))
                self.out.append(('final', finals.pop(0)))
                self.t += FINAL_US

        load()
        evs1.append(self.take())
        self.spend(DRAIN_US + PAIR_US * len(STEPS[-1]))
        for b, chunks in TURNS:
            for begin, end in PARTS:
                load()
                old = [c for c in range(chunks[0]) if block(c) <= block(chunks[0]) - 2]
                if b:
                    load((chunks[0], end - 1))
                    for i in old if not begin else ():
                        if i not in reused:
                            reused.add(i)
                            for n in SIDES:
                                while ('P', i, n) not in self.arr:
                                    self.advance()
                                self.out.append(('reuse', ('P', i, n)))
                    final()
                else:
                    final(max(old, default=-1))
                evs2.append(self.take())
                self.spend(DRAIN_US + EXPERT_US * GROUP * (end - begin))
            for i in chunks:
                if b:
                    for n in SIDES:
                        self.push(('x', n), self.sum * CHUNKS[i][1], ('P', i, n))
                else:
                    summed.add(i)
            self.poll()
        final(len(CHUNKS))
        return evs1, evs2, self.take(), order


def kernel(side, hid, idx, gate, wg, wu, wd, out, GU, WST, WDB, WDT,
           X, H, own, wbuf, WD, PS, RSB, G, GT, GPT, iv, gv,
           s_in, s_own, s_send, s_link, s_chip, s_way, s_tok, s_gate, s_down, s_dway, s_dchip, s_sum, s_w, s_wd):
    me = lax.axis_index('ep')
    core, x, y = lax.rem(me, 2), lax.rem(me // 2, side), me // (2 * side)
    tokens, d_model = hid.shape
    half, quarter = tokens // 2, tokens // 4
    ff = wd.shape[1]
    kh, fh = d_model // 2, ff // 2
    item = 2
    planner = Planner(kh * BLOCK * item, fh * item, quarter * d_model * item, HELD * half * 4, half * 4)
    evs1, evs2, tail, order = planner.run()
    rank = {p: i for i, p in enumerate(order)}

    def device(dx, dy, dc=0):
        row, col = lax.rem(y + dy + side, side), lax.rem(x + dx + side, side)
        return (row * side + col) * 2 + lax.rem(core + dc, 2)

    near = {to: device(*to) for to in ((1, 0), (-1, 0), (0, 1), (0, -1), (0, 0, 1))}

    def dev(*to):
        return {'ep': near[to]}

    def part(size, i):
        return pl.ds(i * size, size)

    def column(k, d):
        return (0 if d == 1 else 2) + k

    def expert(n, dy, cc=0):
        return ROWS.index(dy) * GROUP + (1 + n) + cc

    def chunk(i):
        c0, w = CHUNKS[i]
        return c0 // BLOCK, pl.ds(c0 % BLOCK, w)

    def down(i, e):
        b, c = chunk(i)
        return WDB.at[b, e, :, c]

    def down_half(i, n, dy, h):
        b, c = chunk(i)
        return WDB.at[b, expert(n, dy), part(fh, h), c]

    def piece(t, k, d, n, h):
        return GU.at[rank[t, k, d, n], 0, part(kh, h)]

    def copy_of(key, sem=None):
        t, i, *rest = key
        if t == 'G':
            n, = rest
            z = (1 - n) // 2
            return GT.at[part(HELD, 1), part(half, z)], GPT.at[:, part(half, z)], s_gate.at[z], (n, 0)
        if t == 'T':
            n, = rest
            z = (1 - n) + i
            return hid.at[part(quarter, z)], X.at[part(quarter, z)], s_tok.at[z], (n, 0)
        if t == 'W':
            d, h = rest
            j = column(i, d)
            return own.at[j, part(kh, h)], WST.at[j, part(kh, h)], s_way.at[j, h], (0, d)
        if t in ('D', 'R', 'S', 'F'):
            d, n, h = rest
            j = column(i, d)
            src, to = {'D': (own.at[j, part(kh, h)], (-n, 0)), 'R': (WST.at[j, part(kh, h)], (-n, 0)),
                       'S': (piece('D', i, d, n, h) if t == 'S' else None, (0, -d)),
                       'F': (piece('R', i, d, n, h) if t == 'F' else None, (0, d))}[t]
            return src, piece(t, i, d, n, h), s_link.at[rank[t, i, d, n], h], to
        if t == 'B':
            a = rank[(i, *rest)]
            return GU.at[a, 0], GU.at[a, 1], s_chip.at[a], (0, 0, 1)
        if t == 'w':
            h, = rest
            b, c = chunk(i)
            c0, w = CHUNKS[i]
            return wd.at[0, part(fh, h), pl.ds(c0, w)], WDT.at[b, part(fh, h), c], s_dway.at[i, h], (0, DIRS[h])
        if t in ('d', 'r', 's', 'f'):
            n, *dy, h = rest
            d = DIRS[h]
            b, c = chunk(i)
            c0, w = CHUNKS[i]
            if t == 'd':
                dy, src, to = 0, wd.at[0, part(fh, h), pl.ds(c0, w)], (-n, 0)
            elif t == 'r':
                dy, src, to = -d, WDT.at[b, part(fh, h), c], (-n, 0)
            elif t == 's':
                dy, = dy
                src, to = down_half(i, n, 0, h), (0, -dy)
            else:
                dy, src, to = 2, down_half(i, n, -d, h), (0, d)
            return src, down_half(i, n, dy, h), s_down.at[i, expert(n, dy) // 2, h], to
        if t == 'b':
            n, dy = rest
            return down(i, expert(n, dy)), down(i, expert(n, dy, 1)), s_dchip.at[i, expert(n, dy) // 2], (0, 0, 1)
        n, = rest
        z = (1 + n) // 2
        b, c = chunk(i)
        return PS.at[1, b % 2, part(half, z), c], RSB.at[b, part(half, z), c], s_sum.at[i, z], (n, 0)

    sends = [key for events in evs1 + evs2 + [tail] for kind, key in events if kind == 'send']
    sent, settled = {key: i for i, key in enumerate(sends)}, set()

    def remote(key):
        src, dst, sem, to = copy_of(key)
        return pltpu.make_async_remote_copy(src, dst, s_send.at[sent[key]], sem, device_id=dev(*to), device_id_type=MESH)

    def stage(j, p):
        return pltpu.make_async_copy((wg, wu)[p].at[0, :, part(LANES, j)], own.at[j, :, part(LANES, p)], s_own.at[j, p])

    def bring(i):
        src, dst = ((hid, out), (idx, iv), (gate, gv))[i]
        return pltpu.make_async_copy(src, dst, s_in.at[i])

    def tall(rows):
        return jnp.concatenate([rows, jnp.zeros((LANES - HELD, tokens), F32)], axis=0).T

    def build_gates():
        bring(1).wait()
        bring(2).wait()
        shape = (2 * HELD, tokens)
        r, t = lax.broadcasted_iota(jnp.int32, shape, 0), lax.broadcasted_iota(jnp.int32, shape, 1)
        e = lax.rem(r, HELD)
        q = e // GROUP
        dy = jnp.where(q == 1, 1, jnp.where(q == 2, -1, jnp.where(q == 3, 2, 0)))
        shift = jnp.where(r < HELD, 0, jnp.where(t < half, 1, -1)) + 2 * lax.rem(e // 2, 2) - 1
        row, col = lax.rem(y + dy + side, side), lax.rem(x + shift + side, side)
        ids = (row * side + col) * 2 + lax.rem(core + e, 2)
        acc = jnp.zeros(shape, F32)
        for c in range(idx.shape[0]):
            acc = acc + jnp.where(iv[c:c + 1, :] == ids, gv[c:c + 1, :], 0)
        GT[...] = acc
        G[0] = tall(acc[:HELD])

    flags = set()

    def first_time(name):
        new = name not in flags
        flags.add(name)
        return new

    def load_down(par, g, b, c, sub):
        return pltpu.make_async_copy(WDB.at[b, part(GROUP, g), :, c], WD.at[par, part(GROUP, g), :, c], s_wd.at[par, g, sub])

    def emit(events):
        for kind, key in events:
            if kind == 'send':
                t, k, d, *_ = key
                if t in ('D', 'W') and first_time(column(k, d)):
                    for p in BOTH:
                        stage(column(k, d), p).wait()
                if t == 'G' and first_time('gates'):
                    build_gates()
                remote(key).start()
            elif kind == 'wait':
                _, dst, sem, _ = copy_of(key)
                pltpu.make_async_copy(dst, dst, sem).wait()
                if key[0] == 'G' and not first_time('partner'):
                    G[1] = tall(GPT[...])
            elif kind == 'load':
                i, g = key
                b, c = chunk(i)
                load_down(b % 2, g, b, c, CHUNKS[i][0] % BLOCK // LANES).start()
            elif kind in ('reuse', 'settle'):
                remote(key).wait_send()
                settled.add(key)
            else:
                c0, w = CHUNKS[key]
                b, c = chunk(key)
                for r in range(0, tokens, BLOCK):
                    rows = pl.ds(r, BLOCK)
                    out[rows, pl.ds(c0, w)] = (PS[0, b % 2, rows, c] + RSB[b, rows, c]).astype(BF16)

    barrier = pltpu.get_barrier_semaphore()
    for to in near:
        pl.semaphore_signal(barrier, inc=1, device_id=dev(*to), device_id_type=MESH)
    for k in BOTH:
        for d in DIRS:
            for p in BOTH:
                stage(column(k, d), p).start()
    for i in (1, 2, 0):
        bring(i).start()
    pl.semaphore_wait(barrier, len(near))

    def ffn_in(b, a, slot, j):
        rows_in = (out, X)[b]
        for cc in BOTH:
            for r in range(0, tokens, BLOCK):
                rows = pl.ds(r, BLOCK)
                ab = jnp.dot(rows_in[rows, :], wbuf[slot, j, cc], preferred_element_type=F32)
                u = ab[:, :LANES]
                H[b, a, cc, rows, :] = (u * jax.nn.sigmoid(u) * ab[:, LANES:]).astype(BF16)

    def load_piece(a, slot, j):
        return pltpu.make_async_copy(GU.at[a], wbuf.at[slot, j], s_w.at[slot, j])

    def indices(pattern, it, base):
        return [base[ch] + it * pattern.count(ch) + pattern[:j].count(ch) for j, ch in enumerate(pattern)]

    def load_pieces(pattern, it, base, slot):
        for j, a in enumerate(indices(pattern, it, base)):
            load_piece(a, slot, j).start()

    emit(evs1[0])
    bring(0).wait()
    first, base = 0, {'o': 0, 'p': 0}
    load_pieces(STEPS[0], 0, base, 0)
    for si, (pattern, count) in enumerate(SEGMENTS):
        after = {ch: base[ch] + pattern.count(ch) * count for ch in base}
        follow = SEGMENTS[si + 1][0] if si + 1 < len(SEGMENTS) else None

        def body(it, _, first=first, base=base, pattern=pattern, count=count, after=after, follow=follow):
            slot, other = lax.rem(first + it, 2), lax.rem(first + it + 1, 2)
            for v in range(count):
                if ev := evs1[first + v + 1]:
                    pl.when(it == v)(lambda ev=ev: emit(ev))
            pl.when(it < count - 1)(lambda: load_pieces(pattern, it + 1, base, other))
            if follow:
                pl.when(it == count - 1)(lambda: load_pieces(follow, 0, after, other))
            mine = indices(pattern, it, base)
            for j, a in enumerate(mine):
                load_piece(a, slot, j).wait()
            for j, (ch, a) in enumerate(zip(pattern, mine)):
                ffn_in(0 if ch == 'o' else 1, a, slot, j)
            return 0

        lax.fori_loop(0, count, body, 0)
        first, base = first + count, after

    def held(n, dy):
        near_d, far_d = {0: 'DD', 1: 'SR', -1: 'RS', 2: 'FF'}[dy]
        return [rank[near_d, k, 1, n] for k in BOTH] + [rank[far_d, k, -1, n] for k in BOTH]

    def ffn_out(b, par, g, c):
        for q in range(GROUP):
            n, cc = SIDES[q // 2], q % 2
            e = g * GROUP + q
            for r in range(0, tokens, BLOCK):
                rows = pl.ds(r, BLOCK)
                hh = jnp.concatenate([H[b, a, cc, rows, :] for a in held(n, ROWS[g])], axis=1)
                o = jnp.dot(hh, WD[par, e, :, c], preferred_element_type=F32).astype(BF16).astype(F32)
                ge = G[b, rows, e:e + 1]
                v = jnp.where(ge > 0, ge * o, 0)
                PS[b, par, rows, c] = v if e == 0 else PS[b, par, rows, c] + v

    def sums(b, par, c, sub, turns, v):
        for z, (begin, end) in enumerate(PARTS):
            for u in turns:
                if ev := evs2[u * len(PARTS) + z]:
                    pl.when(v == u)(lambda ev=ev: emit(ev))

            @pl.when(b == 1)
            def _():
                for g in range(begin, end):
                    load_down(par, g, 0, c, sub).wait()

            for g in range(begin, end):
                ffn_out(b, par, g, c)

    whole = [u for u, (_, chunks) in enumerate(TURNS) if CHUNKS[chunks[0]][1] == BLOCK]
    parts = [u for u, (b, _) in enumerate(TURNS) if b and u not in whole]
    last = len(TURNS) - 1
    par = block(len(CHUNKS) - 1) % 2

    def body_whole(v, _):
        sums(1 - lax.rem(v, 2), lax.rem(v // 2, 2), pl.ds(0, BLOCK), 0, whole, v)
        return 0

    def body_parts(v, _):
        sub = v - len(whole)
        sums(1, par, pl.ds(pl.multiple_of(sub * LANES, LANES), LANES), sub, parts, v)
        return 0

    lax.fori_loop(0, len(whole), body_whole, 0)
    lax.fori_loop(len(whole), last, body_parts, 0)
    sums(0, par, pl.ds(0, BLOCK), 0, (last,), last)
    for key in sent:
        if key not in settled and key[0] != 'P':
            remote(key).wait_send()
            settled.add(key)
    emit([event for event in tail if event[0] != 'settle'])
    for key in sent:
        if key not in settled:
            remote(key).wait_send()


def solution(mesh):
    side = math.isqrt(mesh.shape['ep'] // 2)

    def device_body(hidden, route_idx, gate_weights, w_gate, w_up, w_down):
        tokens, d_model = hidden.shape
        ff = w_gate.shape[2]
        top_k = route_idx.shape[1]
        blocks, nc = d_model // BLOCK, len(CHUNKS)
        shape = jax.ShapeDtypeStruct
        anywhere = pl.BlockSpec(memory_space=pl.ANY)
        dma = pltpu.SemaphoreType.DMA
        columns = ff // LANES
        pairs = HELD // 2
        return pl.pallas_call(
            lambda *refs: kernel(side, *refs),
            out_shape=[pltpu.VMEM((tokens, d_model), BF16), shape((PIECES, 2, d_model, BLOCK), BF16),
                       shape((columns, d_model, BLOCK), BF16), shape((blocks, HELD, ff, BLOCK), BF16),
                       shape((blocks, ff, BLOCK), BF16)],
            in_specs=[anywhere] * 6,
            out_specs=[pl.BlockSpec(memory_space=pltpu.VMEM)] + [anywhere] * 4,
            scratch_shapes=[
                pltpu.VMEM((tokens, d_model), BF16),
                pltpu.VMEM((2, PIECES, 2, tokens, LANES), BF16),
                pltpu.VMEM((columns, d_model, BLOCK), BF16),
                pltpu.VMEM((2, 3, 2, d_model, BLOCK), BF16),
                pltpu.VMEM((2, HELD, ff, BLOCK), BF16),
                pltpu.VMEM((2, 2, tokens, BLOCK), F32),
                pltpu.VMEM((blocks, tokens, BLOCK), F32),
                pltpu.VMEM((2, tokens, LANES), F32),
                pltpu.VMEM((2 * HELD, tokens), F32),
                pltpu.VMEM((HELD, tokens), F32),
                pltpu.VMEM((top_k, tokens), jnp.int32),
                pltpu.VMEM((top_k, tokens), F32),
                dma((3,)), dma((columns, 2)), dma((256,)), dma((PIECES, 2)), dma((PIECES,)), dma((columns, 2)), dma((4,)),
                dma((2,)), dma((nc, pairs, 2)), dma((nc, 2)), dma((nc, pairs)), dma((nc, 2)), dma((2, 3)), dma((2, GROUP, 2)),
            ],
            compiler_params=pltpu.CompilerParams(collective_id=0, has_side_effects=True, vmem_limit_bytes=VMEM_BYTES),
            name='moe',
        )(hidden, route_idx.T, gate_weights.T, w_gate, w_up, w_down)[0]

    row_spec = P(('dp', 'ep'), None)
    expert_spec = P('ep', None, None)
    return jax.shard_map(device_body, mesh=mesh, in_specs=(row_spec,) * 3 + (expert_spec,) * 3, out_specs=row_spec, check_vma=False)
```
